256 devices in a mesh: grp: 4 (over z_lo), tp: 32 (over x, y, z_hi), rep: 2 (over core).
Axes of the slice: x: 4, y: 4, z: 8 (z_hi: 2, z_lo: 4; z = z_hi * 4 + z_lo), core: 2. Of those that a mesh axis runs over, the one named last changes fastest.
Arguments:
- query_rows: bfloat16 [32, 1024, 2048], P('tp', ('grp', 'rep')), may hold values from -120 to 120
- key_rows: bfloat16 [32, 1024, 512], P('tp', ('grp', 'rep')), may hold values from -6 to 6, as said below
- value_rows: bfloat16 [32, 1024, 512], P('tp', ('grp', 'rep')), may hold values from -6 to 6
- teacher_codes: bfloat16 [32, 1024, 4096], P(None, ('grp', 'rep'), 'tp'), may hold values from -6 to 6
- teacher_scales: bfloat16 [32, 1024, 32], P(None, ('grp', 'rep'), 'tp'), may hold values from 0.099609375 to 1
- projection: bfloat16 [2048, 4096], P(None, ('grp', 'rep')), may hold values from -0.125 to 0.125
Outputs:
- grad_query: bfloat16 [32, 1024, 2048], P('tp', ('grp', 'rep'))
- grad_key: bfloat16 [32, 1024, 512], P('tp', ('grp', 'rep'))
- grad_value: bfloat16 [32, 1024, 512], P('tp', ('grp', 'rep'))
The draws below stay inside these ranges and needn't reach their ends.
Inputs may be any that keep to these rules, and one draw needn't show every extreme that they name: `key_rows`: keys of every head.
All inputs are finite; a program needn't handle non-finite values.
Results may differ from the reference program's by a relative error of at most 0.014.
Values may be sent and summed in bfloat16 or wider, within the bound.
No kernel may reach another device: no remote copies, remote signals or barrier semaphores. Data moves between devices by JAX's collectives and lax.ppermute only.
A program may use at most 128 MiB of HBM per device.

```python
import math
import jax
import jax.numpy as jnp
from jax import lax

TOK_DEV = 128
HEADS = 16
KV_HEADS = 4
HEAD_DIM = 128
COLS = 4096
QBLOCK = 128
SEQS = 32
SEQ_LEN = 1024
N_GRP = 4
N_REP = 2


def paired_fields(key):
    query_noise = jax.random.normal(jax.random.fold_in(key, 101), (SEQS, SEQ_LEN, HEADS, HEAD_DIM), jnp.float32)
    key_noise = jax.random.normal(jax.random.fold_in(key, 202), (SEQS, SEQ_LEN, KV_HEADS, HEAD_DIM), jnp.float32)
    keys_field = jnp.clip(key_noise, -6.0, 6.0)
    queries_field = jnp.clip(2.0 * query_noise, -12.0, 12.0)
    queries_field = queries_field.reshape(SEQS, SEQ_LEN, HEADS * HEAD_DIM)
    keys_field = keys_field.reshape(SEQS, SEQ_LEN, KV_HEADS * HEAD_DIM)
    return (queries_field, keys_field)


def draw_query_rows(key, part):
    return paired_fields(key)[0].astype(jnp.bfloat16)


def draw_key_rows(key, part):
    return paired_fields(key)[1].astype(jnp.bfloat16)


def block_levels(stream_key, dims, shards, least, top_value):
    gain, own = 1.0, jax.random.fold_in(stream_key, 6)
    for axis_at, parts in shards:
        draws = jnp.exp(jax.random.uniform(jax.random.fold_in(own, axis_at), (parts,), jnp.float32, least / len(shards), top_value / len(shards)))
        gain = gain * jnp.repeat(draws, dims[axis_at] // parts).reshape([-1 if axis == axis_at else 1 for axis in range(len(dims))])
    return gain


def bell_draw(own_key, dims, width, reach, shards=(), kind=jnp.bfloat16):
    array = width * jax.random.normal(own_key, dims, jnp.float32)
    if shards:
        array = array * block_levels(own_key, dims, shards, -0.22, 0.18)
    return jnp.clip(array, -reach, reach).astype(kind)


def setup_inputs(seed: int = 0) -> dict:
    splits = jax.random.split(jax.random.key(seed), 7)
    return {
        "query_rows": draw_query_rows(jax.random.fold_in(splits[6], 71), 0),
        "key_rows": draw_key_rows(jax.random.fold_in(splits[6], 71), 0),
        "value_rows": bell_draw(splits[2], (SEQS, SEQ_LEN, KV_HEADS * HEAD_DIM), 1.0, 6.0, ((0, 32), (1, 8))),
        "teacher_codes": bell_draw(splits[3], (SEQS, SEQ_LEN, COLS), 1.0, 6.0, ((1, 8), (2, 32))),
        "teacher_scales": jnp.clip(jnp.exp(math.log(1.0) - 2.306499 * jax.random.uniform(splits[4], (SEQS, SEQ_LEN, COLS // QBLOCK), jnp.float32) ** block_levels(splits[4], (SEQS, SEQ_LEN, COLS // QBLOCK), ((1, 8), (2, 32)), -0.2, 0.2)), 0.099609375, 1.0).astype(jnp.bfloat16),
        "projection": bell_draw(splits[5], (HEADS * HEAD_DIM, COLS), (HEADS * HEAD_DIM) ** -0.5, 0.125, ((1, 8),)),
    }


masked_low = -1e+30

def reference(query_rows, key_rows, value_rows, teacher_codes, teacher_scales, projection):
    group_size = HEADS // KV_HEADS
    part_count = N_GRP * N_REP
    col_width = COLS // part_count
    block_count = SEQ_LEN // TOK_DEV
    inv_root = 1.0 / math.sqrt(HEAD_DIM)
    row_ids = jnp.arange(TOK_DEV, dtype=jnp.int32)
    col_ids = jnp.arange(SEQ_LEN, dtype=jnp.int32)
    highest = lax.Precision.HIGHEST

    def one_slab(slab_data):
        slab_query, slab_key, slab_value, slab_codes, slab_scales = slab_data
        key_heads = slab_key.reshape(SEQ_LEN, KV_HEADS, HEAD_DIM).transpose(1, 0, 2).astype(jnp.float32)
        value_heads = slab_value.reshape(SEQ_LEN, KV_HEADS, HEAD_DIM).transpose(1, 0, 2).astype(jnp.float32)

        def scan_step(running, block_index):
            grad_keys, grad_values = running
            first = (block_index * TOK_DEV).astype(jnp.int32)
            query_part = lax.dynamic_slice_in_dim(slab_query, first, TOK_DEV, 0)
            queries = query_part.reshape(TOK_DEV, KV_HEADS, group_size, HEAD_DIM).transpose(1, 2, 0, 3).astype(jnp.float32)
            raw_scores = jnp.einsum('hgqd,hkd->hgqk', queries, key_heads, precision=highest) * inv_root
            allowed = col_ids[None, :] <= (first + row_ids)[:, None]
            scores = jnp.where(allowed, raw_scores, masked_low)
            row_peak = scores.max(-1)
            shifted = jnp.exp(scores - row_peak[..., None])
            row_total = shifted.sum(-1)
            probs = shifted / row_total[..., None]
            prob_low = probs.astype(jnp.bfloat16)
            attn_wide = jnp.einsum('hgqk,hkd->hgqd', prob_low.astype(jnp.float32), value_heads, precision=highest)
            attn_flat = attn_wide.transpose(2, 0, 1, 3).reshape(TOK_DEV, HEADS * HEAD_DIM)
            attn_low = attn_flat.astype(jnp.bfloat16)
            approx = jnp.dot(attn_low, projection, preferred_element_type=jnp.float32)
            code_rows = lax.dynamic_slice_in_dim(slab_codes, first, TOK_DEV, 0).astype(jnp.float32)
            scale_rows = lax.dynamic_slice_in_dim(slab_scales, first, TOK_DEV, 0).astype(jnp.float32)
            target = (code_rows.reshape(TOK_DEV, COLS // QBLOCK, QBLOCK) * scale_rows[..., None]).reshape(TOK_DEV, COLS)
            errors = (approx - target).astype(jnp.bfloat16)
            grad_attn = jnp.zeros((TOK_DEV, HEADS * HEAD_DIM), jnp.float32)
            for column_block in range(part_count):
                lower = column_block * col_width
                term = jnp.dot(errors[:, lower:lower + col_width], projection[:, lower:lower + col_width].T, preferred_element_type=jnp.float32)
                term_low = lax.optimization_barrier(term.astype(jnp.bfloat16))
                grad_attn = grad_attn + term_low.astype(jnp.float32)
            grad_low = grad_attn.astype(jnp.bfloat16)
            grad_heads = grad_low.reshape(TOK_DEV, KV_HEADS, group_size, HEAD_DIM).transpose(1, 2, 0, 3).astype(jnp.float32)
            row_delta = (grad_heads * attn_wide).sum(-1)
            grad_prob = jnp.einsum('hgqd,hkd->hgqk', grad_heads, value_heads, precision=highest)
            grad_score = (probs * (grad_prob - row_delta[..., None]) * inv_root).astype(jnp.bfloat16).astype(jnp.float32)
            grad_queries = jnp.einsum('hgqk,hkd->hgqd', grad_score, key_heads, precision=highest)
            grad_queries = grad_queries.transpose(2, 0, 1, 3).reshape(TOK_DEV, HEADS * HEAD_DIM).astype(jnp.bfloat16)
            key_piece = jnp.einsum('hgqk,hgqd->hkd', grad_score, queries, precision=highest)
            value_piece = jnp.einsum('hgqk,hgqd->hkd', prob_low.astype(jnp.float32), grad_heads, precision=highest)
            key_low = lax.optimization_barrier(key_piece.astype(jnp.bfloat16))
            value_low = lax.optimization_barrier(value_piece.astype(jnp.bfloat16))
            grad_keys = grad_keys + key_low.astype(jnp.float32)
            grad_values = grad_values + value_low.astype(jnp.float32)
            return ((grad_keys, grad_values), grad_queries)
        zeros_kv = jnp.zeros((KV_HEADS, SEQ_LEN, HEAD_DIM), jnp.float32)
        (grad_keys, grad_values), grad_queries = lax.scan(scan_step, (zeros_kv, zeros_kv), jnp.arange(block_count, dtype=jnp.int32))
        grad_queries = grad_queries.reshape(SEQ_LEN, HEADS * HEAD_DIM)
        grad_keys = grad_keys.transpose(1, 0, 2).reshape(SEQ_LEN, KV_HEADS * HEAD_DIM).astype(jnp.bfloat16)
        grad_values = grad_values.transpose(1, 0, 2).reshape(SEQ_LEN, KV_HEADS * HEAD_DIM).astype(jnp.bfloat16)
        return (grad_queries, grad_keys, grad_values)
    grad_query, grad_key, grad_value = lax.map(one_slab, (query_rows, key_rows, value_rows, teacher_codes, teacher_scales))
    return (grad_query, grad_key, grad_value)
```

```python
import math

import jax
import jax.numpy as jnp
from jax import lax
from jax.experimental import pallas as pl
from jax.experimental.pallas import tpu as pltpu
from jax.sharding import PartitionSpec as P

HEADS = 16
KV_HEADS = 4
GROUP = HEADS // KV_HEADS
HD = 128
ROWS = 128
FEAT = HEADS * HD
INV_ROOT = 1.0 / math.sqrt(HD)
LOW = -1e30
N_GRP = 4
SLOTS = 8


SWAP = [(0, 1), (1, 0)]


def tp_of(x, y, zh):
    return x * 8 + y * 2 + zh


def x_shift(d):
    return [(tp_of(x, y, h), tp_of((x + d) % 4, y, h)) for x in range(4) for y in range(4) for h in range(2)]


def y_shift(d):
    return [(tp_of(x, y, h), tp_of(x, (y + d) % 4, h)) for x in range(4) for y in range(4) for h in range(2)]


def z_shift(d):
    def at(x, y, z):
        return (z % 4) * 32 + tp_of(x, y, z // 4)

    return [(at(x, y, z), at(x, y, (z + d) % 8)) for x in range(4) for y in range(4) for z in range(8)]


def up(d):
    return [(i, i + d) for i in range(N_GRP - d)]


def down(d):
    return [(i + d, i) for i in range(N_GRP - d)]


def nt(a, b):
    return lax.dot_general(a, b, (((1,), (1,)), ((), ())), preferred_element_type=jnp.float32)


def nn(a, b):
    return lax.dot_general(a, b, (((1,), (0,)), ((), ())), preferred_element_type=jnp.float32)


def tn(a, b):
    return lax.dot_general(a, b, (((0,), (0,)), ((), ())), preferred_element_type=jnp.float32)


def stack_heads(block):
    return jnp.concatenate([block[:, g * HD : (g + 1) * HD] for g in range(GROUP)], axis=0)


def spread_heads(rows):
    return jnp.concatenate([rows[g * ROWS : (g + 1) * ROWS] for g in range(GROUP)], axis=1)


def forward_body(info, q, *refs):
    pieces, (wide, low, probs) = refs[:SLOTS], refs[SLOTS:]
    grp, rep = info[0], info[1]
    q4 = stack_heads(q[...])
    keys = jnp.concatenate([p[0] for p in pieces], axis=0)
    values = jnp.concatenate([p[1] for p in pieces], axis=0)
    scores = nt(q4, keys) * INV_ROOT
    row = lax.broadcasted_iota(jnp.int32, (GROUP * ROWS, ROWS), 0) % ROWS
    col = lax.broadcasted_iota(jnp.int32, (GROUP * ROWS, ROWS), 1)
    parts = []
    for s in range(SLOTS):
        d, other = s // 2, s % 2
        part = scores[:, s * ROWS : (s + 1) * ROWS]
        if s == 0:
            part = jnp.where(col <= row, part, LOW)
        else:
            seen = rep == 1 if s == 1 else grp >= d
            part = jnp.where(seen, part, LOW)
        parts.append(part)
    scores = jnp.concatenate(parts, axis=1)
    peak = scores.max(axis=1, keepdims=True)
    shifted = jnp.exp(scores - peak)
    total = shifted.sum(axis=1, keepdims=True)
    prob_low = (shifted * (1.0 / total)).astype(jnp.bfloat16)
    probs[...] = prob_low
    out = spread_heads(nn(prob_low, values))
    wide[...] = out
    low[...] = out.astype(jnp.bfloat16)


def forward(info, q, pieces):
    return pl.pallas_call(
        forward_body,
        grid_spec=pltpu.PrefetchScalarGridSpec(
            num_scalar_prefetch=1,
            grid=(KV_HEADS,),
            in_specs=[pl.BlockSpec((ROWS, GROUP * HD), lambda h, i: (0, h))]
            + [pl.BlockSpec((2, ROWS, HD), lambda h, i: (0, 0, h))] * SLOTS,
            out_specs=[
                pl.BlockSpec((ROWS, GROUP * HD), lambda h, i: (0, h)),
                pl.BlockSpec((ROWS, GROUP * HD), lambda h, i: (0, h)),
                pl.BlockSpec((None, GROUP * ROWS, SLOTS * ROWS), lambda h, i: (h, 0, 0)),
            ],
        ),
        out_shape=[
            jax.ShapeDtypeStruct((ROWS, FEAT), jnp.float32),
            jax.ShapeDtypeStruct((ROWS, FEAT), jnp.bfloat16),
            jax.ShapeDtypeStruct((KV_HEADS, GROUP * ROWS, SLOTS * ROWS), jnp.bfloat16),
        ],
        cost_estimate=pl.CostEstimate(flops=10**10, bytes_accessed=8 * 10**6, transcendentals=2 * 10**6),
        name="attn_fwd",
    )(info, q, *pieces)


def project_body(info, mine, theirs, target_mine, target_theirs, own, *refs):
    arrays, (part_mine, part_theirs), (weights, both, acc, sems) = refs[:8], refs[8:10], refs[10:]
    grp, rep, xi, yi = info[0], info[1], info[2], info[3]
    copies = [pltpu.make_async_copy(own, weights.at[3], sems.at[32])]
    copies[0].start()
    for a in range(8):
        half, far = a // 4, a % 4
        for s in range(4):
            dx, dy = (s, far) if half == 0 else (far, s)
            head = ((xi + 4 - dx) % 4) * 4 + (yi + 4 - dy) % 4
            rows = pl.ds(pl.multiple_of(head * HD, HD), HD)
            c = pltpu.make_async_copy(
                arrays[a].at[s], weights.at[pl.ds(0, 3), rows, pl.ds(half * 256, 256)], sems.at[a * 4 + s]
            )
            c.start()
            copies.append(c)
    both[0:ROWS] = mine[...]
    both[ROWS:] = theirs[...]
    for n, (j, shift) in enumerate(((3, 0), (0, 3), (1, 1), (2, 2))):
        if n == 0:
            copies[0].wait()
        if n == 1:
            for c in copies[1:]:
                c.wait()
        block = (grp + shift) % 4
        approx = nn(both[...], weights[j])
        target = jnp.concatenate(
            [
                jnp.concatenate([target_mine[block, rep, c], target_theirs[block, c]], axis=0)
                for c in range(4)
            ],
            axis=1,
        )
        errors = (approx - target.astype(jnp.float32)).astype(jnp.bfloat16)
        term = nt(errors, weights[j])
        if n == 0:
            acc[...] = term
        else:
            acc[...] += term
    part_mine[...] = acc[0:ROWS]
    part_theirs[...] = acc[ROWS:].astype(jnp.bfloat16)


def project(info, mine, theirs, target_mine, target_theirs, own, arrays):
    vmem = pl.BlockSpec(memory_space=pltpu.VMEM)
    hbm = pl.BlockSpec(memory_space=pltpu.HBM)
    return pl.pallas_call(
        project_body,
        grid_spec=pltpu.PrefetchScalarGridSpec(
            num_scalar_prefetch=1,
            grid=(1,),
            in_specs=[vmem] * 4 + [hbm] * 9,
            out_specs=[vmem, vmem],
            scratch_shapes=[
                pltpu.VMEM((4, FEAT, 512), jnp.bfloat16),
                pltpu.VMEM((2 * ROWS, FEAT), jnp.bfloat16),
                pltpu.VMEM((2 * ROWS, FEAT), jnp.float32),
                pltpu.SemaphoreType.DMA((33,)),
            ],
        ),
        out_shape=[
            jax.ShapeDtypeStruct((ROWS, FEAT), jnp.float32),
            jax.ShapeDtypeStruct((ROWS, FEAT), jnp.bfloat16),
        ],
        cost_estimate=pl.CostEstimate(flops=10**10, bytes_accessed=12 * 10**6, transcendentals=0),
        name="project",
    )(info, mine, theirs, target_mine, target_theirs, own, *arrays)


def backward_body(probs, part, got, wide, q, *refs):
    pieces, (grad_q, terms_mine, terms_theirs) = refs[:SLOTS], refs[SLOTS:]
    grad = (part[...] + got[...].astype(jnp.float32)).astype(jnp.bfloat16)
    delta = stack_heads(grad.astype(jnp.float32) * wide[...]).sum(axis=1, keepdims=True)
    g4 = stack_heads(grad)
    q4 = stack_heads(q[...])
    keys = jnp.concatenate([p[0] for p in pieces], axis=0)
    values = jnp.concatenate([p[1] for p in pieces], axis=0)
    p_low = probs[...]
    grad_prob = nt(g4, values)
    grad_score = (p_low.astype(jnp.float32) * (grad_prob - delta) * INV_ROOT).astype(jnp.bfloat16)
    grad_q[...] = spread_heads(nn(grad_score, keys)).astype(jnp.bfloat16)
    key_terms = tn(grad_score, q4).astype(jnp.bfloat16)
    value_terms = tn(p_low, g4).astype(jnp.bfloat16)
    for s in range(SLOTS):
        out = terms_theirs if s % 2 else terms_mine
        out[s // 2, 0] = key_terms[s * ROWS : (s + 1) * ROWS]
        out[s // 2, 1] = value_terms[s * ROWS : (s + 1) * ROWS]


def backward(probs, part, got, wide, q, pieces):
    rows = pl.BlockSpec((ROWS, GROUP * HD), lambda h: (0, h))
    terms = pl.BlockSpec((N_GRP, 2, ROWS, HD), lambda h: (0, 0, 0, h))
    return pl.pallas_call(
        backward_body,
        grid=(KV_HEADS,),
        in_specs=[pl.BlockSpec((None, GROUP * ROWS, SLOTS * ROWS), lambda h: (h, 0, 0)), rows, rows, rows, rows]
        + [pl.BlockSpec((2, ROWS, HD), lambda h: (0, 0, h))] * SLOTS,
        out_specs=[rows, terms, terms],
        out_shape=[
            jax.ShapeDtypeStruct((ROWS, FEAT), jnp.bfloat16),
            jax.ShapeDtypeStruct((N_GRP, 2, ROWS, KV_HEADS * HD), jnp.bfloat16),
            jax.ShapeDtypeStruct((N_GRP, 2, ROWS, KV_HEADS * HD), jnp.bfloat16),
        ],
        cost_estimate=pl.CostEstimate(flops=10**10, bytes_accessed=8 * 10**6, transcendentals=0),
        name="attn_bwd",
    )(probs, part, got, wide, q, *pieces)


def spread_weights(projection, xi, yi):
    part = lax.dynamic_slice_in_dim(projection, (xi * 4 + yi) * HD, HD, 0)
    from_z = [lax.ppermute(part, ("grp", "tp"), z_shift(d)) for d in (1, 7, 6)]
    arrays = []
    for half, (near, far) in enumerate(((x_shift, y_shift), (y_shift, x_shift))):
        slab = jnp.stack([a[:, half * 256 : half * 256 + 256] for a in from_z])
        row = jnp.stack([slab] + [lax.ppermute(slab, "tp", near(d)) for d in (1, 2, 3)])
        arrays += [row] + [lax.ppermute(row, "tp", far(d)) for d in (1, 2, 3)]
    return arrays


def shards(query_rows, key_rows, value_rows, teacher_codes, teacher_scales, projection):
    grp, rep, tp = lax.axis_index("grp"), lax.axis_index("rep"), lax.axis_index("tp")
    xi, yi = tp // 8, (tp // 2) % 4
    info = jnp.stack([grp, rep, xi, yi]).astype(jnp.int32)
    query = query_rows[0]

    with jax.named_scope("weights"):
        arrays = spread_weights(projection, xi, yi)
    with jax.named_scope("keys"):
        mine = jnp.concatenate([key_rows, value_rows], axis=0)
        mine = [mine] + [lax.ppermute(mine, "grp", up(d)) for d in (1, 2, 3)]
        pieces = []
        for piece in mine:
            pieces += [piece, lax.ppermute(piece, "rep", SWAP)]
    with jax.named_scope("teacher"):
        rows = (teacher_codes.astype(jnp.float32) * teacher_scales.astype(jnp.float32)).astype(jnp.bfloat16)
        rows = lax.all_to_all(rows, "tp", split_axis=0, concat_axis=0, tiled=True)
        target_mine = rows.reshape(N_GRP, 2, 4, ROWS, HD)
        give = lax.dynamic_index_in_dim(target_mine, 1 - rep, 1, keepdims=False)
        target_theirs = lax.ppermute(give, "rep", SWAP)

    wide, low, probs = forward(info, query, pieces)
    theirs = lax.ppermute(low, "rep", SWAP)
    part, give = project(info, low, theirs, target_mine, target_theirs, projection, arrays)
    got = lax.ppermute(give, "rep", SWAP)
    grad_q, terms_mine, terms_theirs = backward(probs, part, got, wide, query, pieces)
    got = lax.ppermute(terms_theirs, "rep", SWAP)
    terms = [terms_mine[d].astype(jnp.float32) + got[d].astype(jnp.float32) for d in range(N_GRP)]
    total = terms[0]
    for d in (1, 2, 3):
        total = total + lax.ppermute(terms[d].astype(jnp.bfloat16), "grp", down(d)).astype(jnp.float32)
    total = total.astype(jnp.bfloat16)
    return grad_q[None], total[0:1], total[1:2]


def solution(mesh):
    rows = P("tp", ("grp", "rep"), None)
    cols = P(None, ("grp", "rep"), "tp")
    return jax.shard_map(
        shards,
        mesh=mesh,
        in_specs=(rows, rows, rows, cols, cols, P(None, ("grp", "rep"))),
        out_specs=(rows, rows, rows),
        check_vma=False,
    )
```

```python
import math

import jax
import jax.numpy as jnp
from jax import lax
from jax.experimental import pallas as pl
from jax.experimental.pallas import tpu as pltpu
from jax.sharding import PartitionSpec as P


HEADS = 16
KV_HEADS = 4
GROUP = HEADS // KV_HEADS
HD = 128
ROWS = 128
FEAT = HEADS * HD
INV_ROOT = 1.0 / math.sqrt(HD)
LOW = -1e30
N_GRP = 4
SLOTS = 8
QUARTER = FEAT // 4
EIGHTH = FEAT // 8


SWAP = [(0, 1), (1, 0)]


def tp_of(x, y, zh):
    return x * 8 + y * 2 + zh


def x_shift(d):
    return [(tp_of(x, y, h), tp_of((x + d) % 4, y, h)) for x in range(4) for y in range(4) for h in range(2)]


def y_shift(d):
    return [(tp_of(x, y, h), tp_of(x, (y + d) % 4, h)) for x in range(4) for y in range(4) for h in range(2)]


X_PAIR = [(t, t ^ 8) for t in range(32)]
Y_PAIR = [(t, t ^ 2) for t in range(32)]


def z_shift(d):
    def at(x, y, z):
        return (z % 4) * 32 + tp_of(x, y, z // 4)

    return [(at(x, y, z), at(x, y, (z + d) % 8)) for x in range(4) for y in range(4) for z in range(8)]


def up(d):
    return [(i, i + d) for i in range(N_GRP - d)]


def down(d):
    return [(i + d, i) for i in range(N_GRP - d)]


def nt(a, b):
    return lax.dot_general(a, b, (((1,), (1,)), ((), ())), preferred_element_type=jnp.float32)


def nn(a, b):
    return lax.dot_general(a, b, (((1,), (0,)), ((), ())), preferred_element_type=jnp.float32)


def tn(a, b):
    return lax.dot_general(a, b, (((0,), (0,)), ((), ())), preferred_element_type=jnp.float32)


def stack_heads(block):
    return jnp.concatenate([block[:, g * HD : (g + 1) * HD] for g in range(GROUP)], axis=0)


def spread_heads(rows):
    return jnp.concatenate([rows[g * ROWS : (g + 1) * ROWS] for g in range(GROUP)], axis=1)


def forward_body(info, q, *refs):
    pieces, (wide, low, probs) = refs[:SLOTS], refs[SLOTS:]
    grp, rep = info[0], info[1]
    q4 = stack_heads(q[...])
    keys = jnp.concatenate([p[0] for p in pieces], axis=0)
    values = jnp.concatenate([p[1] for p in pieces], axis=0)
    scores = nt(q4, keys) * INV_ROOT
    row = lax.broadcasted_iota(jnp.int32, (GROUP * ROWS, ROWS), 0) % ROWS
    col = lax.broadcasted_iota(jnp.int32, (GROUP * ROWS, ROWS), 1)
    parts = []
    for s in range(SLOTS):
        d = s // 2
        part = scores[:, s * ROWS : (s + 1) * ROWS]
        if s == 0:
            part = jnp.where(col <= row, part, LOW)
        else:
            seen = rep == 1 if s == 1 else grp >= d
            part = jnp.where(seen, part, LOW)
        parts.append(part)
    scores = jnp.concatenate(parts, axis=1)
    peak = scores.max(axis=1, keepdims=True)
    shifted = jnp.exp(scores - peak)
    total = shifted.sum(axis=1, keepdims=True)
    prob_low = (shifted * (1.0 / total)).astype(jnp.bfloat16)
    probs[...] = prob_low
    out = spread_heads(nn(prob_low, values))
    wide[...] = out
    low[...] = out.astype(jnp.bfloat16)


def forward(info, q, pieces):
    return pl.pallas_call(
        forward_body,
        grid_spec=pltpu.PrefetchScalarGridSpec(
            num_scalar_prefetch=1,
            grid=(KV_HEADS,),
            in_specs=[pl.BlockSpec((ROWS, GROUP * HD), lambda h, i: (0, h))]
            + [pl.BlockSpec((2, ROWS, HD), lambda h, i: (0, 0, h))] * SLOTS,
            out_specs=[
                pl.BlockSpec((ROWS, GROUP * HD), lambda h, i: (0, h)),
                pl.BlockSpec((ROWS, GROUP * HD), lambda h, i: (0, h)),
                pl.BlockSpec((None, GROUP * ROWS, SLOTS * ROWS), lambda h, i: (h, 0, 0)),
            ],
        ),
        out_shape=[
            jax.ShapeDtypeStruct((ROWS, FEAT), jnp.float32),
            jax.ShapeDtypeStruct((ROWS, FEAT), jnp.bfloat16),
            jax.ShapeDtypeStruct((KV_HEADS, GROUP * ROWS, SLOTS * ROWS), jnp.bfloat16),
        ],
        cost_estimate=pl.CostEstimate(flops=10**10, bytes_accessed=8 * 10**6, transcendentals=2 * 10**6),
        name="attn_fwd",
    )(info, q, *pieces)


def project_body(info, mine, theirs, target_mine, target_theirs, own, *refs):
    arrays, (part_mine, part_theirs), (weights, both, acc, sems) = refs[:8], refs[8:10], refs[10:]
    grp, rep, xi, yi, zh = info[0], info[1], info[2], info[3], info[4]
    copies = [pltpu.make_async_copy(own, weights.at[3], sems.at[16])]
    copies[0].start()
    for a in range(8):
        half, far = a // 4, a % 4
        part = ((xi if half else yi) + 4 - far) % 4
        for k in range(2):
            sub = ((yi if half else xi) + k) % 2
            rows = pl.ds(pl.multiple_of(part * QUARTER + sub * EIGHTH, EIGHTH), EIGHTH)
            c = pltpu.make_async_copy(
                arrays[a].at[k], weights.at[pl.ds(0, 3), rows, pl.ds(half * 256, 256)], sems.at[2 * a + k]
            )
            c.start()
            copies.append(c)
    both[0:ROWS] = mine[...]
    both[ROWS:] = theirs[...]
    for n, (j, shift) in enumerate(((3, 0), (0, 3), (1, 1), (2, 2))):
        if n == 0:
            copies[0].wait()
        if n == 1:
            for c in copies[1:]:
                c.wait()
        block = (grp + shift) % 4
        approx = nn(both[...], weights[j])
        target = jnp.concatenate(
            [
                jnp.concatenate(
                    [target_mine[(c + zh) % 2, block, rep, c // 2], target_theirs[(c + zh) % 2, block, c // 2]], axis=0
                )
                for c in range(4)
            ],
            axis=1,
        )
        errors = (approx - target.astype(jnp.float32)).astype(jnp.bfloat16)
        term = nt(errors, weights[j])
        if n == 0:
            acc[...] = term
        else:
            acc[...] += term
    part_mine[...] = acc[0:ROWS]
    part_theirs[...] = acc[ROWS:].astype(jnp.bfloat16)


def project(info, mine, theirs, target_mine, target_theirs, own, arrays):
    vmem = pl.BlockSpec(memory_space=pltpu.VMEM)
    hbm = pl.BlockSpec(memory_space=pltpu.HBM)
    return pl.pallas_call(
        project_body,
        grid_spec=pltpu.PrefetchScalarGridSpec(
            num_scalar_prefetch=1,
            grid=(1,),
            in_specs=[vmem] * 4 + [hbm] * 9,
            out_specs=[vmem, vmem],
            scratch_shapes=[
                pltpu.VMEM((4, FEAT, 512), jnp.bfloat16),
                pltpu.VMEM((2 * ROWS, FEAT), jnp.bfloat16),
                pltpu.VMEM((2 * ROWS, FEAT), jnp.float32),
                pltpu.SemaphoreType.DMA((17,)),
            ],
        ),
        out_shape=[
            jax.ShapeDtypeStruct((ROWS, FEAT), jnp.float32),
            jax.ShapeDtypeStruct((ROWS, FEAT), jnp.bfloat16),
        ],
        cost_estimate=pl.CostEstimate(flops=10**10, bytes_accessed=12 * 10**6, transcendentals=0),
        name="project",
    )(info, mine, theirs, target_mine, target_theirs, own, *arrays)


def backward_body(probs, part, got, wide, q, *refs):
    pieces, (grad_q, terms_mine, terms_theirs) = refs[:SLOTS], refs[SLOTS:]
    grad = (part[...] + got[...].astype(jnp.float32)).astype(jnp.bfloat16)
    delta = stack_heads(grad.astype(jnp.float32) * wide[...]).sum(axis=1, keepdims=True)
    g4 = stack_heads(grad)
    q4 = stack_heads(q[...])
    keys = jnp.concatenate([p[0] for p in pieces], axis=0)
    values = jnp.concatenate([p[1] for p in pieces], axis=0)
    p_low = probs[...]
    grad_prob = nt(g4, values)
    grad_score = (p_low.astype(jnp.float32) * (grad_prob - delta) * INV_ROOT).astype(jnp.bfloat16)
    grad_q[...] = spread_heads(nn(grad_score, keys)).astype(jnp.bfloat16)
    key_terms = tn(grad_score, q4).astype(jnp.bfloat16)
    value_terms = tn(p_low, g4).astype(jnp.bfloat16)
    for s in range(SLOTS):
        out = terms_theirs if s % 2 else terms_mine
        out[s // 2, 0] = key_terms[s * ROWS : (s + 1) * ROWS]
        out[s // 2, 1] = value_terms[s * ROWS : (s + 1) * ROWS]


def backward(probs, part, got, wide, q, pieces):
    rows = pl.BlockSpec((ROWS, GROUP * HD), lambda h: (0, h))
    terms = pl.BlockSpec((N_GRP, 2, ROWS, HD), lambda h: (0, 0, 0, h))
    return pl.pallas_call(
        backward_body,
        grid=(KV_HEADS,),
        in_specs=[pl.BlockSpec((None, GROUP * ROWS, SLOTS * ROWS), lambda h: (h, 0, 0)), rows, rows, rows, rows]
        + [pl.BlockSpec((2, ROWS, HD), lambda h: (0, 0, h))] * SLOTS,
        out_specs=[rows, terms, terms],
        out_shape=[
            jax.ShapeDtypeStruct((ROWS, FEAT), jnp.bfloat16),
            jax.ShapeDtypeStruct((N_GRP, 2, ROWS, KV_HEADS * HD), jnp.bfloat16),
            jax.ShapeDtypeStruct((N_GRP, 2, ROWS, KV_HEADS * HD), jnp.bfloat16),
        ],
        cost_estimate=pl.CostEstimate(flops=10**10, bytes_accessed=8 * 10**6, transcendentals=0),
        name="attn_bwd",
    )(probs, part, got, wide, q, *pieces)


def spread_weights(projection, xi, yi):
    places = ((yi, xi % 2), (xi, yi % 2))
    parts = [
        lax.dynamic_slice(projection, (at * QUARTER + sub * EIGHTH, half * 256), (EIGHTH, 256))
        for half, (at, sub) in enumerate(places)
    ]
    below, above = [lax.ppermute(jnp.stack(parts), ("grp", "tp"), z_shift(d)) for d in (1, 7)]
    across = [lax.ppermute(part, ("grp", "tp"), z_shift(d)) for part, d in zip(parts, (2, 6))]
    arrays = []
    for half, (pair, far) in enumerate(((X_PAIR, y_shift), (Y_PAIR, x_shift))):
        slab = jnp.stack([below[half], above[half], across[half]])
        other = lax.ppermute(slab, "tp", pair)
        slab = jnp.stack([slab, other])
        arrays += [slab] + [lax.ppermute(slab, "tp", far(d)) for d in (1, 2, 3)]
    return arrays


def join_body(keys, values, out):
    out[0:1] = keys[...]
    out[1:2] = values[...]


def gather_keys(key_rows, value_rows, give):
    piece = pl.pallas_call(
        join_body, out_shape=jax.ShapeDtypeStruct((2, ROWS, KV_HEADS * HD), jnp.bfloat16), name="join"
    )(key_rows, value_rows)
    pieces = []
    for d in range(N_GRP):
        if d == 3:
            piece, give = lax.optimization_barrier((piece, give))
        if d:
            piece = lax.ppermute(piece, "grp", up(1))
        pieces += [piece, lax.ppermute(piece, "rep", SWAP)]
    return pieces, give


def step(query_rows, key_rows, value_rows, teacher_codes, teacher_scales, projection):
    grp, rep, tp = lax.axis_index("grp"), lax.axis_index("rep"), lax.axis_index("tp")
    xi, yi, zh = tp // 8, (tp // 2) % 4, tp % 2
    info = jnp.stack([grp, rep, xi, yi, zh]).astype(jnp.int32)
    query = query_rows[0]

    arrays = spread_weights(projection, xi, yi)
    rows = (teacher_codes.astype(jnp.float32) * teacher_scales.astype(jnp.float32)).astype(jnp.bfloat16)
    rows = rows.reshape(16, 2, ROWS, HD)
    rows = lax.all_to_all(
        rows,
        "tp",
        split_axis=0,
        concat_axis=0,
        tiled=True,
        axis_index_groups=[[2 * t + h for t in range(16)] for h in range(2)],
    )
    keep = lax.dynamic_index_in_dim(rows, zh, 1, keepdims=False)
    give = lax.dynamic_index_in_dim(rows, 1 - zh, 1, keepdims=False)
    pieces, give = gather_keys(key_rows, value_rows, give)
    got = lax.ppermute(give, "tp", [(t, t ^ 1) for t in range(32)])
    target_mine = jnp.stack([keep, got]).reshape(2, N_GRP, 2, 2, ROWS, HD)
    give = lax.dynamic_index_in_dim(target_mine, 1 - rep, 2, keepdims=False)
    target_theirs = lax.ppermute(give, "rep", SWAP)

    wide, low, probs = forward(info, query, pieces)
    theirs = lax.ppermute(low, "rep", SWAP)
    part, give = project(info, low, theirs, target_mine, target_theirs, projection, arrays)
    got = lax.ppermute(give, "rep", SWAP)
    grad_q, terms_mine, terms_theirs = backward(probs, part, got, wide, query, pieces)
    got = lax.ppermute(terms_theirs, "rep", SWAP)
    terms = [terms_mine[d].astype(jnp.float32) + got[d].astype(jnp.float32) for d in range(N_GRP)]
    low_terms = [t.astype(jnp.bfloat16) for t in terms]
    relayed = lax.ppermute(low_terms[3], "grp", [(3, 2)])
    near = lax.ppermute(low_terms[1], "grp", down(1))
    far = lax.ppermute(low_terms[2], "grp", [(3, 1)])
    joined = (terms[2] + relayed.astype(jnp.float32)).astype(jnp.bfloat16)
    joined = lax.ppermute(joined, "grp", [(2, 0)])
    total = terms[0] + near.astype(jnp.float32) + far.astype(jnp.float32) + joined.astype(jnp.float32)
    total = total.astype(jnp.bfloat16)
    return grad_q[None], total[0:1], total[1:2]


def solution(mesh):
    rows = P("tp", ("grp", "rep"), None)
    cols = P(None, ("grp", "rep"), "tp")
    return jax.shard_map(
        step,
        mesh=mesh,
        in_specs=(rows, rows, rows, cols, cols, P(None, ("grp", "rep"))),
        out_specs=(rows, rows, rows),
        check_vma=False,
    )
```

```python
import math

import jax
import jax.numpy as jnp
from jax import lax
from jax.experimental import pallas as pl
from jax.experimental.pallas import tpu as pltpu
from jax.sharding import PartitionSpec as P


HEADS = 16
KV_HEADS = 4
GROUP = HEADS // KV_HEADS
HD = 128
ROWS = 128
FEAT = HEADS * HD
INV_ROOT = 1.0 / math.sqrt(HD)
LOW = -1e30
N_GRP = 4
SLOTS = 8
QUARTER = FEAT // 4
EIGHTH = FEAT // 8


SWAP = [(0, 1), (1, 0)]


def tp_of(x, y, zh):
    return x * 8 + y * 2 + zh


def x_shift(d):
    return [(tp_of(x, y, h), tp_of((x + d) % 4, y, h)) for x in range(4) for y in range(4) for h in range(2)]


def y_shift(d):
    return [(tp_of(x, y, h), tp_of(x, (y + d) % 4, h)) for x in range(4) for y in range(4) for h in range(2)]


X_PAIR = [(t, t ^ 8) for t in range(32)]
Y_PAIR = [(t, t ^ 2) for t in range(32)]


def z_shift(d):
    def at(x, y, z):
        return (z % 4) * 32 + tp_of(x, y, z // 4)

    return [(at(x, y, z), at(x, y, (z + d) % 8)) for x in range(4) for y in range(4) for z in range(8)]


def up(d):
    return [(i, i + d) for i in range(N_GRP - d)]


def down(d):
    return [(i + d, i) for i in range(N_GRP - d)]


def nt(a, b):
    return lax.dot_general(a, b, (((1,), (1,)), ((), ())), preferred_element_type=jnp.float32)


def nn(a, b):
    return lax.dot_general(a, b, (((1,), (0,)), ((), ())), preferred_element_type=jnp.float32)


def tn(a, b):
    return lax.dot_general(a, b, (((0,), (0,)), ((), ())), preferred_element_type=jnp.float32)


def stack_heads(block):
    return jnp.concatenate([block[:, g * HD : (g + 1) * HD] for g in range(GROUP)], axis=0)


def spread_heads(rows):
    return jnp.concatenate([rows[g * ROWS : (g + 1) * ROWS] for g in range(GROUP)], axis=1)


def kv_lanes(h):
    return pl.ds(pl.multiple_of(h * HD, HD), HD), pl.ds(pl.multiple_of(h * GROUP * HD, GROUP * HD), GROUP * HD)


VMEM_SPEC = pl.BlockSpec(memory_space=pltpu.VMEM)
HBM_SPEC = pl.BlockSpec(memory_space=pltpu.HBM)
PARAMS = pltpu.CompilerParams(vmem_limit_bytes=32 * 2**20)


def forward_body(info, q, *refs):
    pieces, (wide, low, probs) = refs[:SLOTS], refs[SLOTS:]
    grp, rep = info[0], info[1]
    head, heads = kv_lanes(pl.program_id(0))
    q4 = stack_heads(q[...])
    keys = jnp.concatenate([p[0, :, head] for p in pieces], axis=0)
    values = jnp.concatenate([p[1, :, head] for p in pieces], axis=0)
    scores = nt(q4, keys) * INV_ROOT
    row = lax.broadcasted_iota(jnp.int32, (GROUP * ROWS, ROWS), 0) % ROWS
    col = lax.broadcasted_iota(jnp.int32, (GROUP * ROWS, ROWS), 1)
    parts = []
    for s in range(SLOTS):
        d = s // 2
        part = scores[:, s * ROWS : (s + 1) * ROWS]
        if s == 0:
            part = jnp.where(col <= row, part, LOW)
        else:
            seen = rep == 1 if s == 1 else grp >= d
            part = jnp.where(seen, part, LOW)
        parts.append(part)
    scores = jnp.concatenate(parts, axis=1)
    peak = scores.max(axis=1, keepdims=True)
    shifted = jnp.exp(scores - peak)
    total = shifted.sum(axis=1, keepdims=True)
    prob_low = (shifted * (1.0 / total)).astype(jnp.bfloat16)
    probs[...] = prob_low
    out = spread_heads(nn(prob_low, values))
    wide[...] = out
    low[:, heads] = out.astype(jnp.bfloat16)


def forward(info, q, pieces):
    return pl.pallas_call(
        forward_body,
        grid_spec=pltpu.PrefetchScalarGridSpec(
            num_scalar_prefetch=1,
            grid=(KV_HEADS,),
            in_specs=[pl.BlockSpec((ROWS, GROUP * HD), lambda h, i: (0, h))]
            + [VMEM_SPEC] * SLOTS,
            out_specs=[
                pl.BlockSpec((ROWS, GROUP * HD), lambda h, i: (0, h)),
                VMEM_SPEC,
                pl.BlockSpec((None, GROUP * ROWS, SLOTS * ROWS), lambda h, i: (h, 0, 0)),
            ],
        ),
        out_shape=[
            jax.ShapeDtypeStruct((ROWS, FEAT), jnp.float32),
            pltpu.VMEM((ROWS, FEAT), jnp.bfloat16),
            jax.ShapeDtypeStruct((KV_HEADS, GROUP * ROWS, SLOTS * ROWS), jnp.bfloat16),
        ],
        compiler_params=PARAMS,
        cost_estimate=pl.CostEstimate(flops=10**10, bytes_accessed=8 * 10**6, transcendentals=2 * 10**6),
        name="attn_fwd",
    )(info, q, *pieces)


def project_body(info, mine, theirs, target_mine, target_theirs, own, *refs):
    arrays, (part_mine, part_theirs), (weights, both, acc, sems) = refs[:8], refs[8:10], refs[10:]
    grp, rep, xi, yi, zh = info[0], info[1], info[2], info[3], info[4]
    copies = [pltpu.make_async_copy(own, weights.at[3], sems.at[16])]
    copies[0].start()
    for a in range(8):
        half, far = a // 4, a % 4
        part = ((xi if half else yi) + 4 - far) % 4
        for k in range(2):
            sub = ((yi if half else xi) + k) % 2
            rows = pl.ds(pl.multiple_of(part * QUARTER + sub * EIGHTH, EIGHTH), EIGHTH)
            c = pltpu.make_async_copy(
                arrays[a].at[k], weights.at[pl.ds(0, 3), rows, pl.ds(half * 256, 256)], sems.at[2 * a + k]
            )
            c.start()
            copies.append(c)
    both[0:ROWS] = mine[...]
    both[ROWS:] = theirs[...]
    for n, (j, shift) in enumerate(((3, 0), (0, 3), (1, 1), (2, 2))):
        if n == 0:
            copies[0].wait()
        if n == 1:
            for c in copies[1:]:
                c.wait()
        block = (grp + shift) % 4
        approx = nn(both[...], weights[j])
        target = jnp.concatenate(
            [
                jnp.concatenate(
                    [target_mine[(c + zh) % 2, block, rep, c // 2], target_theirs[(c + zh) % 2, block, c // 2]], axis=0
                )
                for c in range(4)
            ],
            axis=1,
        )
        errors = (approx - target.astype(jnp.float32)).astype(jnp.bfloat16)
        term = nt(errors, weights[j])
        if n == 0:
            acc[...] = term
        else:
            acc[...] += term
    part_mine[...] = acc[0:ROWS]
    part_theirs[...] = acc[ROWS:].astype(jnp.bfloat16)


def project(info, mine, theirs, target_mine, target_theirs, own, arrays):
    vmem = pl.BlockSpec(memory_space=pltpu.VMEM)
    hbm = pl.BlockSpec(memory_space=pltpu.HBM)
    return pl.pallas_call(
        project_body,
        grid_spec=pltpu.PrefetchScalarGridSpec(
            num_scalar_prefetch=1,
            grid=(1,),
            in_specs=[vmem] * 4 + [hbm] * 9,
            out_specs=[vmem, vmem],
            scratch_shapes=[
                pltpu.VMEM((4, FEAT, 512), jnp.bfloat16),
                pltpu.VMEM((2 * ROWS, FEAT), jnp.bfloat16),
                pltpu.VMEM((2 * ROWS, FEAT), jnp.float32),
                pltpu.SemaphoreType.DMA((17,)),
            ],
        ),
        out_shape=[pltpu.VMEM((ROWS, FEAT), jnp.float32), pltpu.VMEM((ROWS, FEAT), jnp.bfloat16)],
        compiler_params=PARAMS,
        cost_estimate=pl.CostEstimate(flops=10**10, bytes_accessed=12 * 10**6, transcendentals=0),
        name="project",
    )(info, mine, theirs, target_mine, target_theirs, own, *arrays)


def backward_body(probs, part, got, wide, q, *refs):
    pieces, (grad_q, terms_mine, terms_theirs) = refs[:SLOTS], refs[SLOTS:]
    head, heads = kv_lanes(pl.program_id(0))
    grad = (part[:, heads] + got[:, heads].astype(jnp.float32)).astype(jnp.bfloat16)
    delta = stack_heads(grad.astype(jnp.float32) * wide[...]).sum(axis=1, keepdims=True)
    g4 = stack_heads(grad)
    q4 = stack_heads(q[...])
    keys = jnp.concatenate([p[0, :, head] for p in pieces], axis=0)
    values = jnp.concatenate([p[1, :, head] for p in pieces], axis=0)
    p_low = probs[...]
    grad_prob = nt(g4, values)
    grad_score = (p_low.astype(jnp.float32) * (grad_prob - delta) * INV_ROOT).astype(jnp.bfloat16)
    grad_q[...] = spread_heads(nn(grad_score, keys)).astype(jnp.bfloat16)
    key_terms = tn(grad_score, q4).astype(jnp.bfloat16)
    value_terms = tn(p_low, g4).astype(jnp.bfloat16)
    for s in range(SLOTS):
        out = terms_theirs if s % 2 else terms_mine
        out[s // 2, 0, :, head] = key_terms[s * ROWS : (s + 1) * ROWS]
        out[s // 2, 1, :, head] = value_terms[s * ROWS : (s + 1) * ROWS]


def backward(probs, part, got, wide, q, pieces):
    rows = pl.BlockSpec((ROWS, GROUP * HD), lambda h: (0, h))
    terms = pltpu.VMEM((N_GRP, 2, ROWS, KV_HEADS * HD), jnp.bfloat16)
    return pl.pallas_call(
        backward_body,
        grid=(KV_HEADS,),
        in_specs=[pl.BlockSpec((None, GROUP * ROWS, SLOTS * ROWS), lambda h: (h, 0, 0)), VMEM_SPEC, VMEM_SPEC, rows, rows]
        + [VMEM_SPEC] * SLOTS,
        out_specs=[rows, VMEM_SPEC, VMEM_SPEC],
        out_shape=[
            jax.ShapeDtypeStruct((ROWS, FEAT), jnp.bfloat16),
            terms,
            terms,
        ],
        compiler_params=PARAMS,
        cost_estimate=pl.CostEstimate(flops=10**10, bytes_accessed=8 * 10**6, transcendentals=0),
        name="attn_bwd",
    )(probs, part, got, wide, q, *pieces)


def spread_weights(projection, xi, yi):
    places = ((yi, xi % 2), (xi, yi % 2))
    parts = [
        lax.dynamic_slice(projection, (at * QUARTER + sub * EIGHTH, half * 256), (EIGHTH, 256))
        for half, (at, sub) in enumerate(places)
    ]
    below, above = [lax.ppermute(jnp.stack(parts), ("grp", "tp"), z_shift(d)) for d in (1, 7)]
    across = [lax.ppermute(part, ("grp", "tp"), z_shift(d)) for part, d in zip(parts, (2, 6))]
    arrays = []
    for half, (pair, far) in enumerate(((X_PAIR, y_shift), (Y_PAIR, x_shift))):
        slab = jnp.stack([below[half], above[half], across[half]])
        other = lax.ppermute(slab, "tp", pair)
        slab = jnp.stack([slab, other])
        arrays += [slab] + [lax.ppermute(slab, "tp", far(d)) for d in (1, 2, 3)]
    return arrays


def join_body(keys, values, out):
    out[0:1] = keys[...]
    out[1:2] = values[...]


def gather_keys(key_rows, value_rows, give):
    piece = pl.pallas_call(
        join_body, out_shape=jax.ShapeDtypeStruct((2, ROWS, KV_HEADS * HD), jnp.bfloat16), name="join"
    )(key_rows, value_rows)
    pieces = []
    for d in range(N_GRP):
        if d == 3:
            piece, give = lax.optimization_barrier((piece, give))
        if d:
            piece = lax.ppermute(piece, "grp", up(1))
        pieces += [piece, lax.ppermute(piece, "rep", SWAP)]
    return pieces, give


def step(query_rows, key_rows, value_rows, teacher_codes, teacher_scales, projection):
    grp, rep, tp = lax.axis_index("grp"), lax.axis_index("rep"), lax.axis_index("tp")
    xi, yi, zh = tp // 8, (tp // 2) % 4, tp % 2
    info = jnp.stack([grp, rep, xi, yi, zh]).astype(jnp.int32)
    query = query_rows[0]

    arrays = spread_weights(projection, xi, yi)
    rows = (teacher_codes.astype(jnp.float32) * teacher_scales.astype(jnp.float32)).astype(jnp.bfloat16)
    rows = rows.reshape(16, 2, ROWS, HD)
    rows = lax.all_to_all(
        rows,
        "tp",
        split_axis=0,
        concat_axis=0,
        tiled=True,
        axis_index_groups=[[2 * t + h for t in range(16)] for h in range(2)],
    )
    keep = lax.dynamic_index_in_dim(rows, zh, 1, keepdims=False)
    give = lax.dynamic_index_in_dim(rows, 1 - zh, 1, keepdims=False)
    pieces, give = gather_keys(key_rows, value_rows, give)
    got = lax.ppermute(give, "tp", [(t, t ^ 1) for t in range(32)])
    target_mine = jnp.stack([keep, got]).reshape(2, N_GRP, 2, 2, ROWS, HD)
    give = lax.dynamic_index_in_dim(target_mine, 1 - rep, 2, keepdims=False)
    target_theirs = lax.ppermute(give, "rep", SWAP)

    pieces = [pltpu.with_memory_space_constraint(a, pltpu.VMEM) for a in pieces]
    wide, low, probs = forward(info, query, pieces)
    theirs = lax.ppermute(low, "rep", SWAP)
    theirs, target_mine, target_theirs = [
        pltpu.with_memory_space_constraint(a, pltpu.VMEM) for a in (theirs, target_mine, target_theirs)
    ]
    part, give = project(info, low, theirs, target_mine, target_theirs, projection, arrays)
    got = lax.ppermute(give, "rep", SWAP)
    got = pltpu.with_memory_space_constraint(got, pltpu.VMEM)
    grad_q, terms_mine, terms_theirs = backward(probs, part, got, wide, query, pieces)
    got = lax.ppermute(terms_theirs, "rep", SWAP)
    terms = [terms_mine[d].astype(jnp.float32) + got[d].astype(jnp.float32) for d in range(N_GRP)]
    low_terms = [t.astype(jnp.bfloat16) for t in terms]
    relayed = lax.ppermute(low_terms[3], "grp", [(3, 2)])
    near = lax.ppermute(low_terms[1], "grp", down(1))
    far = lax.ppermute(low_terms[2], "grp", [(3, 1)])
    joined = (terms[2] + relayed.astype(jnp.float32)).astype(jnp.bfloat16)
    joined = lax.ppermute(joined, "grp", [(2, 0)])
    total = terms[0] + near.astype(jnp.float32) + far.astype(jnp.float32) + joined.astype(jnp.float32)
    total = total.astype(jnp.bfloat16)
    return grad_q[None], total[0:1], total[1:2]


def solution(mesh):
    rows = P("tp", ("grp", "rep"), None)
    cols = P(None, ("grp", "rep"), "tp")
    return jax.shard_map(
        step,
        mesh=mesh,
        in_specs=(rows, rows, rows, cols, cols, P(None, ("grp", "rep"))),
        out_specs=(rows, rows, rows),
        check_vma=False,
    )
```

```python
import math

import jax
import jax.numpy as jnp
from jax import lax
from jax.experimental import pallas as pl
from jax.experimental.pallas import tpu as pltpu
from jax.sharding import PartitionSpec as P


HEADS = 16
KV_HEADS = 4
GROUP = HEADS // KV_HEADS
HD = 128
ROWS = 128
FEAT = HEADS * HD
INV_ROOT = 1.0 / math.sqrt(HD)
LOW = -1e30
N_GRP = 4
SLOTS = 8
QUARTER = FEAT // 4
EIGHTH = FEAT // 8


SWAP = [(0, 1), (1, 0)]


def tp_of(x, y, zh):
    return x * 8 + y * 2 + zh


def x_shift(d):
    return [(tp_of(x, y, h), tp_of((x + d) % 4, y, h)) for x in range(4) for y in range(4) for h in range(2)]


def y_shift(d):
    return [(tp_of(x, y, h), tp_of(x, (y + d) % 4, h)) for x in range(4) for y in range(4) for h in range(2)]


X_PAIR = [(t, t ^ 8) for t in range(32)]
Y_PAIR = [(t, t ^ 2) for t in range(32)]


def z_shift(d):
    def at(x, y, z):
        return (z % 4) * 32 + tp_of(x, y, z // 4)

    return [(at(x, y, z), at(x, y, (z + d) % 8)) for x in range(4) for y in range(4) for z in range(8)]


def up(d):
    return [(i, i + d) for i in range(N_GRP - d)]


def down(d):
    return [(i + d, i) for i in range(N_GRP - d)]


def nt(a, b):
    return lax.dot_general(a, b, (((1,), (1,)), ((), ())), preferred_element_type=jnp.float32)


def nn(a, b):
    return lax.dot_general(a, b, (((1,), (0,)), ((), ())), preferred_element_type=jnp.float32)


def tn(a, b):
    return lax.dot_general(a, b, (((0,), (0,)), ((), ())), preferred_element_type=jnp.float32)


def stack_heads(block):
    return jnp.concatenate([block[:, g * HD : (g + 1) * HD] for g in range(GROUP)], axis=0)


def spread_heads(rows):
    return jnp.concatenate([rows[g * ROWS : (g + 1) * ROWS] for g in range(GROUP)], axis=1)


def kv_lanes(h):
    return pl.ds(pl.multiple_of(h * HD, HD), HD), pl.ds(pl.multiple_of(h * GROUP * HD, GROUP * HD), GROUP * HD)


VMEM_SPEC = pl.BlockSpec(memory_space=pltpu.VMEM)
HBM_SPEC = pl.BlockSpec(memory_space=pltpu.HBM)
PARAMS = pltpu.CompilerParams(vmem_limit_bytes=32 * 2**20)


def forward_body(info, q, *refs):
    pieces, (wide, low, probs) = refs[:SLOTS], refs[SLOTS:]
    grp, rep = info[0], info[1]
    head, heads = kv_lanes(pl.program_id(0))
    q4 = stack_heads(q[...])
    keys = jnp.concatenate([p[0, :, head] for p in pieces], axis=0)
    values = jnp.concatenate([p[1, :, head] for p in pieces], axis=0)
    scores = nt(q4, keys) * INV_ROOT
    row = lax.broadcasted_iota(jnp.int32, (GROUP * ROWS, ROWS), 0) % ROWS
    col = lax.broadcasted_iota(jnp.int32, (GROUP * ROWS, ROWS), 1)
    parts = []
    for s in range(SLOTS):
        d = s // 2
        part = scores[:, s * ROWS : (s + 1) * ROWS]
        if s == 0:
            part = jnp.where(col <= row, part, LOW)
        else:
            seen = rep == 1 if s == 1 else grp >= d
            part = jnp.where(seen, part, LOW)
        parts.append(part)
    scores = jnp.concatenate(parts, axis=1)
    peak = scores.max(axis=1, keepdims=True)
    shifted = jnp.exp(scores - peak)
    total = shifted.sum(axis=1, keepdims=True)
    prob_low = (shifted * (1.0 / total)).astype(jnp.bfloat16)
    probs[...] = prob_low
    out = spread_heads(nn(prob_low, values))
    wide[...] = out
    low[:, heads] = out.astype(jnp.bfloat16)


def forward(info, q, pieces):
    return pl.pallas_call(
        forward_body,
        grid_spec=pltpu.PrefetchScalarGridSpec(
            num_scalar_prefetch=1,
            grid=(KV_HEADS,),
            in_specs=[pl.BlockSpec((ROWS, GROUP * HD), lambda h, i: (0, h))]
            + [VMEM_SPEC] * SLOTS,
            out_specs=[
                pl.BlockSpec((ROWS, GROUP * HD), lambda h, i: (0, h)),
                VMEM_SPEC,
                pl.BlockSpec((None, GROUP * ROWS, SLOTS * ROWS), lambda h, i: (h, 0, 0)),
            ],
        ),
        out_shape=[
            jax.ShapeDtypeStruct((ROWS, FEAT), jnp.float32),
            pltpu.VMEM((ROWS, FEAT), jnp.bfloat16),
            jax.ShapeDtypeStruct((KV_HEADS, GROUP * ROWS, SLOTS * ROWS), jnp.bfloat16),
        ],
        compiler_params=PARAMS,
        cost_estimate=pl.CostEstimate(flops=10**10, bytes_accessed=8 * 10**6, transcendentals=2 * 10**6),
        name="attn_fwd",
    )(info, q, *pieces)


def project_body(info, mine, theirs, kept, got, target_theirs, own, *refs):
    arrays, (part_mine, part_theirs), (weights, both, acc, sems) = refs[:8], refs[8:10], refs[10:]
    grp, rep, xi, yi, zh = info[0], info[1], info[2], info[3], info[4]
    copies = [pltpu.make_async_copy(own, weights.at[3], sems.at[16])]
    copies[0].start()
    for a in range(8):
        half, far = a // 4, a % 4
        part = ((xi if half else yi) + 4 - far) % 4
        for k in range(2):
            sub = ((yi if half else xi) + k) % 2
            rows = pl.ds(pl.multiple_of(part * QUARTER + sub * EIGHTH, EIGHTH), EIGHTH)
            c = pltpu.make_async_copy(
                arrays[a].at[k], weights.at[pl.ds(0, 3), rows, pl.ds(half * 256, 256)], sems.at[2 * a + k]
            )
            c.start()
            copies.append(c)
    both[0:ROWS] = mine[...]
    both[ROWS:] = theirs[...]
    for n, (j, shift) in enumerate(((3, 0), (0, 3), (1, 1), (2, 2))):
        if n == 0:
            copies[0].wait()
        if n == 1:
            for c in copies[1:]:
                c.wait()
        block = (grp + shift) % 4
        approx = nn(both[...], weights[j])
        target = jnp.concatenate(
            [
                jnp.concatenate(
                    [
                        jnp.where(zh == c % 2, kept[block, rep, c // 2], got[block, rep, c // 2]),
                        target_theirs[(c + zh) % 2, block, c // 2],
                    ],
                    axis=0,
                )
                for c in range(4)
            ],
            axis=1,
        )
        errors = (approx - target.astype(jnp.float32)).astype(jnp.bfloat16)
        term = nt(errors, weights[j])
        if n == 0:
            acc[...] = term
        else:
            acc[...] += term
    part_mine[...] = acc[0:ROWS]
    part_theirs[...] = acc[ROWS:].astype(jnp.bfloat16)


def project(info, mine, theirs, kept, got, target_theirs, own, arrays):
    vmem = pl.BlockSpec(memory_space=pltpu.VMEM)
    hbm = pl.BlockSpec(memory_space=pltpu.HBM)
    return pl.pallas_call(
        project_body,
        grid_spec=pltpu.PrefetchScalarGridSpec(
            num_scalar_prefetch=1,
            grid=(1,),
            in_specs=[vmem] * 5 + [hbm] * 9,
            out_specs=[vmem, vmem],
            scratch_shapes=[
                pltpu.VMEM((4, FEAT, 512), jnp.bfloat16),
                pltpu.VMEM((2 * ROWS, FEAT), jnp.bfloat16),
                pltpu.VMEM((2 * ROWS, FEAT), jnp.float32),
                pltpu.SemaphoreType.DMA((17,)),
            ],
        ),
        out_shape=[pltpu.VMEM((ROWS, FEAT), jnp.float32), pltpu.VMEM((ROWS, FEAT), jnp.bfloat16)],
        compiler_params=PARAMS,
        cost_estimate=pl.CostEstimate(flops=10**10, bytes_accessed=12 * 10**6, transcendentals=0),
        name="project",
    )(info, mine, theirs, kept, got, target_theirs, own, *arrays)


def backward_body(probs, part, got, wide, q, *refs):
    pieces, (grad_q, terms_mine, terms_theirs) = refs[:SLOTS], refs[SLOTS:]
    head, heads = kv_lanes(pl.program_id(0))
    grad = (part[:, heads] + got[:, heads].astype(jnp.float32)).astype(jnp.bfloat16)
    delta = stack_heads(grad.astype(jnp.float32) * wide[...]).sum(axis=1, keepdims=True)
    g4 = stack_heads(grad)
    q4 = stack_heads(q[...])
    keys = jnp.concatenate([p[0, :, head] for p in pieces], axis=0)
    values = jnp.concatenate([p[1, :, head] for p in pieces], axis=0)
    p_low = probs[...]
    grad_prob = nt(g4, values)
    grad_score = (p_low.astype(jnp.float32) * (grad_prob - delta) * INV_ROOT).astype(jnp.bfloat16)
    grad_q[...] = spread_heads(nn(grad_score, keys)).astype(jnp.bfloat16)
    key_terms = tn(grad_score, q4).astype(jnp.bfloat16)
    value_terms = tn(p_low, g4).astype(jnp.bfloat16)
    for s in range(SLOTS):
        out = terms_theirs if s % 2 else terms_mine
        out[s // 2, 0, :, head] = key_terms[s * ROWS : (s + 1) * ROWS]
        out[s // 2, 1, :, head] = value_terms[s * ROWS : (s + 1) * ROWS]


def backward(probs, part, got, wide, q, pieces):
    rows = pl.BlockSpec((ROWS, GROUP * HD), lambda h: (0, h))
    terms = pltpu.VMEM((N_GRP, 2, ROWS, KV_HEADS * HD), jnp.bfloat16)
    return pl.pallas_call(
        backward_body,
        grid=(KV_HEADS,),
        in_specs=[pl.BlockSpec((None, GROUP * ROWS, SLOTS * ROWS), lambda h: (h, 0, 0)), VMEM_SPEC, VMEM_SPEC, rows, rows]
        + [VMEM_SPEC] * SLOTS,
        out_specs=[rows, VMEM_SPEC, VMEM_SPEC],
        out_shape=[
            jax.ShapeDtypeStruct((ROWS, FEAT), jnp.bfloat16),
            terms,
            terms,
        ],
        compiler_params=PARAMS,
        cost_estimate=pl.CostEstimate(flops=10**10, bytes_accessed=8 * 10**6, transcendentals=0),
        name="attn_bwd",
    )(probs, part, got, wide, q, *pieces)


def spread_weights(projection, xi, yi):
    places = ((yi, xi % 2), (xi, yi % 2))
    parts = [
        lax.dynamic_slice(projection, (at * QUARTER + sub * EIGHTH, half * 256), (EIGHTH, 256))
        for half, (at, sub) in enumerate(places)
    ]
    below, above = [lax.ppermute(jnp.stack(parts), ("grp", "tp"), z_shift(d)) for d in (1, 7)]
    across = [lax.ppermute(part, ("grp", "tp"), z_shift(d)) for part, d in zip(parts, (2, 6))]
    arrays = []
    for half, (pair, far) in enumerate(((X_PAIR, y_shift), (Y_PAIR, x_shift))):
        slab = jnp.stack([below[half], above[half], across[half]])
        other = lax.ppermute(slab, "tp", pair)
        slab = jnp.stack([slab, other])
        arrays += [slab] + [lax.ppermute(slab, "tp", far(d)) for d in (1, 2, 3)]
    return arrays


def join_body(keys, values, out):
    out[0:1] = keys[...]
    out[1:2] = values[...]


def gather_keys(key_rows, value_rows, give):
    piece = pl.pallas_call(
        join_body, out_shape=jax.ShapeDtypeStruct((2, ROWS, KV_HEADS * HD), jnp.bfloat16), name="join"
    )(key_rows, value_rows)
    pieces = []
    for d in range(N_GRP):
        if d == 3:
            piece, give = lax.optimization_barrier((piece, give))
        if d:
            piece = lax.ppermute(piece, "grp", up(1)[d - 1 :])
        pieces += [piece, lax.ppermute(piece, "rep", SWAP)]
    return pieces, give


def step(query_rows, key_rows, value_rows, teacher_codes, teacher_scales, projection):
    grp, rep, tp = lax.axis_index("grp"), lax.axis_index("rep"), lax.axis_index("tp")
    xi, yi, zh = tp // 8, (tp // 2) % 4, tp % 2
    info = jnp.stack([grp, rep, xi, yi, zh]).astype(jnp.int32)
    query = query_rows[0]

    arrays = spread_weights(projection, xi, yi)
    rows = (teacher_codes.astype(jnp.float32) * teacher_scales.astype(jnp.float32)).astype(jnp.bfloat16)
    rows = rows.reshape(16, 2, ROWS, HD)
    rows = lax.all_to_all(
        rows,
        "tp",
        split_axis=0,
        concat_axis=0,
        tiled=True,
        axis_index_groups=[[2 * t + h for t in range(16)] for h in range(2)],
    )
    keep = lax.dynamic_index_in_dim(rows, zh, 1, keepdims=False)
    give = lax.dynamic_index_in_dim(rows, 1 - zh, 1, keepdims=False)
    pieces, give = gather_keys(key_rows, value_rows, give)
    got = lax.ppermute(give, "tp", [(t, t ^ 1) for t in range(32)])
    kept, got = [a.reshape(N_GRP, 2, 2, ROWS, HD) for a in (keep, got)]
    give = jnp.stack([lax.dynamic_index_in_dim(a, 1 - rep, 1, keepdims=False) for a in (kept, got)])
    target_theirs = lax.ppermute(give, "rep", SWAP)

    pieces = [pltpu.with_memory_space_constraint(a, pltpu.VMEM) for a in pieces]
    wide, low, probs = forward(info, query, pieces)
    theirs = lax.ppermute(low, "rep", SWAP)
    theirs, kept, got, target_theirs = [
        pltpu.with_memory_space_constraint(a, pltpu.VMEM) for a in (theirs, kept, got, target_theirs)
    ]
    part, give = project(info, low, theirs, kept, got, target_theirs, projection, arrays)
    got = lax.ppermute(give, "rep", SWAP)
    got = pltpu.with_memory_space_constraint(got, pltpu.VMEM)
    grad_q, terms_mine, terms_theirs = backward(probs, part, got, wide, query, pieces)
    got = lax.ppermute(terms_theirs, "rep", SWAP)
    terms = [terms_mine[d].astype(jnp.float32) + got[d].astype(jnp.float32) for d in range(N_GRP)]
    total = terms[0]
    for d in (3, 2, 1):
        total = total + lax.ppermute(terms[d].astype(jnp.bfloat16), "grp", down(d)).astype(jnp.float32)
    total = total.astype(jnp.bfloat16)
    return grad_q[None], total[0:1], total[1:2]


def solution(mesh):
    rows = P("tp", ("grp", "rep"), None)
    cols = P(None, ("grp", "rep"), "tp")
    return jax.shard_map(
        step,
        mesh=mesh,
        in_specs=(rows, rows, rows, cols, cols, P(None, ("grp", "rep"))),
        out_specs=(rows, rows, rows),
        check_vma=False,
    )
```
